32 devices in a mesh: chan: 4 (over z), tm: 8 (over y, x, core).
Axes of the slice: x: 2, y: 2, z: 4, core: 2. Of those that a mesh axis runs over, the one named last changes fastest.
Arguments:
- trajectory: float32 [512, 8, 4096], P('tm', None, 'chan'), may hold values from -40 to 40
- initial: float32 [8, 4096], P(None, 'chan'), may hold values from -6 to 6
- drive_gate: bfloat16 [512, 8, 4096], P('tm', None, 'chan'), may hold values from -16 to 4
- drive_candidate: bfloat16 [512, 8, 4096], P('tm', None, 'chan'), may hold values from -6 to 6
- gate_weight: bfloat16 [4096, 4096], P('chan'), may hold values from -0.0234375 to 0.0234375
- candidate_weight: bfloat16 [4096, 4096], P('chan'), may hold values from -0.09375 to 0.09375
Outputs:
- newton_states: float32 [512, 8, 4096], P('tm', None, 'chan')
- residual_norm: float32 [], replicated
The draws below stay inside these ranges and needn't reach their ends.
All inputs are finite; a program needn't handle non-finite values.
Results may differ from the reference program's by a relative error of at most 0.0016.
Values may be sent and summed in bfloat16 or wider, within the bound.
A program may use at most 128 MiB of HBM per device.

```python
import jax
import jax.numpy as jnp
from jax import lax

H = 4096
BATCH = 8
TIME_STEP_COUNT = 512


def draw_trajectory(key, part):
    first_key = jax.random.fold_in(jax.random.fold_in(key, 11), 0)
    steps_frac = jnp.arange(TIME_STEP_COUNT, dtype=jnp.float32) / TIME_STEP_COUNT
    units_frac = jnp.arange(H, dtype=jnp.float32) / H
    growth = 0.5 * (4.0 ** steps_frac)[:, None, None] * (2.0 ** units_frac)[None, None, :]
    base = jnp.clip(jax.random.normal(first_key, (TIME_STEP_COUNT, BATCH, H), jnp.float32), -6.0, 6.0)
    values = base * growth
    return jnp.clip(values, -40.0, 40.0).astype(jnp.float32)


def draw_drive_gate(key, part):
    decay_random_key, jitter_random_key, spike_random_key = jax.random.split(jax.random.fold_in(key, 23), 3)
    log_rate = jax.random.uniform(decay_random_key, (H,), jnp.float32, jnp.log(1e-05), jnp.log(0.05))
    noise = 0.5 * jnp.clip(jax.random.normal(jitter_random_key, (TIME_STEP_COUNT, BATCH, H), jnp.float32), -4.0, 4.0)
    rate = jnp.exp(log_rate)
    spike_logits = jnp.log(rate) - jnp.log(1.0 - rate)
    spike_events = jax.random.randint(spike_random_key, (4,), 0, TIME_STEP_COUNT)
    step_values = jnp.arange(TIME_STEP_COUNT)
    spike_flags = jnp.any(step_values[:, None] == spike_events[None, :], axis=1)
    drive_level = jnp.where(spike_flags[:, None, None], -0.85, spike_logits[None, None, :])
    return jnp.clip(drive_level + noise, -16.0, 4.0).astype(jnp.bfloat16)


def shard_levels(stream_key, extent, shards, smallest, largest):
    loudness = 1.0
    for dim, blocks in shards:
        heights = jax.random.uniform(jax.random.fold_in(jax.random.fold_in(stream_key, 6), dim), (blocks,), jnp.float32, smallest / len(shards), largest / len(shards))
        loudness = loudness * jnp.repeat(jnp.exp(heights), extent[dim] // blocks).reshape((-1,) + (1,) * (len(extent) - 1 - dim))
    return loudness


def gaussian(key, dims, scale, most, cuts=(), kind=jnp.bfloat16):
    gain = shard_levels(key, dims, cuts, -0.22, 0.18) if cuts else 1.0
    entries = jax.random.normal(key, dims, jnp.float32) * scale * gain
    return jnp.minimum(jnp.maximum(entries, -most), most).astype(kind)


def setup_inputs(seed: int = 0) -> dict:
    key_list = jax.random.split(jax.random.key(seed), 7)
    return {
        "trajectory": draw_trajectory(jax.random.fold_in(key_list[6], 71), 0),
        "initial": gaussian(key_list[1], (BATCH, H), 1.0, 6.0, ((1, 4),), jnp.float32),
        "drive_gate": draw_drive_gate(jax.random.fold_in(key_list[6], 71), 0),
        "drive_candidate": gaussian(key_list[3], (TIME_STEP_COUNT, BATCH, H), 1.0, 6.0, ((0, 8), (2, 4))),
        "gate_weight": gaussian(key_list[4], (H, H), (16 * H) ** -0.5, 0.0234375, ((0, 4),)),
        "candidate_weight": gaussian(key_list[5], (H, H), H ** -0.5, 0.09375, ((0, 4),)),
    }


def advance(state, inputs):
    state = inputs[0] * state + inputs[1]
    return (state, state)

def reference(trajectory, initial, drive_gate, drive_candidate, gate_weight, candidate_weight):
    previous = jnp.concatenate([initial[None], trajectory[:-1]], 0)
    flat = previous.reshape(-1, H).astype(jnp.bfloat16)
    gate_pre = jnp.dot(flat, gate_weight, preferred_element_type=jnp.float32).reshape(previous.shape) + drive_gate.astype(jnp.float32)
    candidate_pre = jnp.dot(flat, candidate_weight, preferred_element_type=jnp.float32).reshape(previous.shape) + drive_candidate.astype(jnp.float32)
    gate_diagonal = jnp.diagonal(gate_weight).astype(jnp.float32)
    candidate_diagonal = jnp.diagonal(candidate_weight).astype(jnp.float32)
    update = jax.nn.sigmoid(gate_pre)
    candidate = jnp.tanh(candidate_pre)
    mapped = (1.0 - update) * previous + update * candidate
    jacobian = 1.0 - update + update * (1.0 - update) * (candidate - previous) * gate_diagonal + update * (1.0 - candidate * candidate) * candidate_diagonal
    offset = mapped - jacobian * previous
    _, newton_states = lax.scan(advance, initial, (jacobian, offset))
    missing = trajectory - mapped
    residual_norm = jnp.sqrt(jnp.mean(missing * missing) + 1e-06)
    return (newton_states, residual_norm)
```

```python
import functools

import jax
import jax.numpy as jnp
from jax import lax
from jax.experimental import pallas as pl
from jax.experimental.pallas import tpu as pltpu
from jax.sharding import PartitionSpec as P

MESH = pl.DeviceIdType.MESH
BF16 = jnp.bfloat16
F32 = jnp.float32


def kernel(
    nz, nt, chunks, tile,
    traj, init, drive_g, drive_c, gate_w, cand_w,
    out, total,
    wbuf, abuf, prev0, diag, prod, carry, ssq, partner_map, maps, tsums, zsums,
    local_sem, wz_send, wz_recv, wx_send, wx_recv, wc_send, wc_recv,
    a_send, a_recv, row_sem, pm_sem, m_send, m_recv, ts_send, ts_recv, zs_send, zs_recv,
):
    z = lax.axis_index("chan")
    t = lax.axis_index("tm")
    steps, batch, width = traj.shape
    nc = nt // 2
    chip = lax.div(t, 2)
    core = lax.rem(t, 2)
    partner = (z, t + 1 - 2 * core)
    part = width // nt
    weights = (gate_w, cand_w)
    rows = steps * batch // chunks
    chunk_steps = steps // chunks

    def remote(src, dst, send, recv, device):
        return pltpu.make_async_remote_copy(
            src_ref=src, dst_ref=dst, send_sem=send, recv_sem=recv,
            device_id=device, device_id_type=MESH,
        )

    def zmod(v):
        return lax.rem(v + 2 * nz, nz)

    def cmod(v):
        return lax.rem(v + 2 * nc, nc)

    def wslot(g, source, p):
        return wbuf.at[g, pl.ds(pl.multiple_of(source * width + p * part, 16), part), :]

    barrier = pltpu.get_barrier_semaphore()
    for d in range(1, nz):
        pl.semaphore_signal(barrier, inc=1, device_id=(zmod(z + d), t), device_id_type=MESH)
    for d in range(1, nt):
        pl.semaphore_signal(barrier, inc=1, device_id=(z, lax.rem(t + d, nt)), device_id_type=MESH)
    pl.semaphore_wait(barrier, nz - 1 + nt - 1)

    sent = []

    def row_copy():
        return remote(traj.at[steps - 1], prev0, row_sem.at[0], row_sem.at[1], (z, lax.rem(t + 1, nt)))

    row_copy().start()

    def z_copy(d, g):
        other = zmod(z + d)
        src = weights[g].at[
            pl.ds(pl.multiple_of(t * part, 16), part), pl.ds(pl.multiple_of(other * width, 128), width)
        ]
        return remote(src, wslot(g, z, t), wz_send.at[g, d - 1], wz_recv.at[g, d - 1], (other, t))

    for d in range(1, nz):
        for g in range(2):
            z_copy(d, g).start()

    def own_copy(g):
        return pltpu.make_async_copy(
            weights[g].at[:, pl.ds(pl.multiple_of(z * width, 128), width)],
            wbuf.at[g, pl.ds(pl.multiple_of(z * width, 128), width), :],
            local_sem.at[g],
        )

    for g in range(2):
        own_copy(g).start()

    own_columns = pl.ds(pl.multiple_of(z * width, 128), width)

    @pl.loop(1, steps // 2)
    def _(j):
        pair = traj[pl.ds(2 * j - 1, 2)].reshape(2 * batch, width)
        abuf[pl.ds(pl.multiple_of(j * 2 * batch, 16), 2 * batch), own_columns] = pair.astype(BF16)

    row_copy().wait()

    @pl.when(t == 0)
    def _():
        prev0[...] = init[...]

    first = jnp.concatenate([prev0[...], traj[0]], 0)
    abuf[pl.ds(0, 2 * batch), own_columns] = first.astype(BF16)

    def a_copy(direction, source, i):
        slot = abuf.at[pl.ds(i * rows, rows), pl.ds(pl.multiple_of(source * width, 128), width)]
        to = z + 1 if direction == 0 else z - 1
        return remote(slot, slot, a_send.at[direction, source, i], a_recv.at[source, i], (to, t))

    for i in range(chunks):
        @pl.when(z < nz - 1)
        def _():
            a_copy(0, z, i).start()

        @pl.when(z > 0)
        def _():
            a_copy(1, z, i).start()

    for g in range(2):
        own_copy(g).wait()
        for j in range(width // 128):
            block = wbuf[g, pl.ds(pl.multiple_of(z * width + j * 128, 128), 128), pl.ds(j * 128, 128)]
            eye = lax.broadcasted_iota(jnp.int32, (128, 128), 0) == lax.broadcasted_iota(
                jnp.int32, (128, 128), 1
            )
            line = jnp.sum(jnp.where(eye, block.astype(F32), 0.0), axis=0, keepdims=True)
            diag[g, :, pl.ds(j * 128, 128)] = jnp.broadcast_to(line, (batch, 128))

    carry[0] = jnp.ones((batch, width), F32)
    carry[1] = jnp.zeros((batch, width), F32)
    ssq[...] = jnp.zeros((batch, width), F32)

    def x_copy(d, g, dq):
        slot = wslot(g, zmod(z - d), t)
        return remote(
            slot, slot, wx_send.at[g, d - 1, dq - 1], wx_recv.at[g, d - 1, dq - 1],
            (z, 2 * cmod(chip + dq) + core),
        )

    def c_copy(d, g, dq, side):
        slot = wslot(g, zmod(z - d), 2 * cmod(chip - dq) + side)
        return remote(slot, slot, wc_send.at[g, d - 1, dq], wc_recv.at[g, d - 1, dq], partner)

    def x_arrival(d, g, dq):
        slot = wslot(g, zmod(z - d), 2 * cmod(chip - dq) + core)
        return remote(slot, slot, wx_send.at[g, d - 1, dq - 1], wx_recv.at[g, d - 1, dq - 1], partner)

    def z_arrival(d, g):
        slot = wslot(g, zmod(z - d), t)
        return remote(slot, slot, wz_send.at[g, d - 1], wz_recv.at[g, d - 1], partner)

    for d in range(1, nz):
        for g in range(2):
            z_arrival(d, g).wait_recv()
            for dq in range(1, nc):
                x_copy(d, g, dq).start()
            c_copy(d, g, 0, core).start()

    onward = [(d, g, dq) for d in range(1, nz) for g in range(2) for dq in range(1, nc)]

    def relay(d, i):
        @pl.when(z - d >= 0)
        def _():
            a_copy(0, z - d, i).wait_recv()

            @pl.when(z < nz - 1)
            def _():
                a_copy(0, z - d, i).start()

        @pl.when(z + d < nz)
        def _():
            a_copy(1, z + d, i).wait_recv()

            @pl.when(z > 0)
            def _():
                a_copy(1, z + d, i).start()

    early = [(d, i) for d in range(1, nz - 1) for i in range(chunks)]
    spread = max(1, (3 * len(early)) // 4)
    per = -(-len(onward) // spread)
    for n, (d, i) in enumerate(early):
        relay(d, i)
        for item in onward[n * per : (n + 1) * per]:
            x_arrival(*item).wait_recv()
            c_copy(*item, core).start()
    for d in range(1, nz):
        for g in range(2):
            for dq in range(nc):
                c_copy(d, g, dq, 1 - core).wait_recv()

    def compute(i):
        @pl.loop(0, width // tile)
        def _(n):
            cols = pl.ds(pl.multiple_of(n * tile, tile), tile)
            lhs = abuf[pl.ds(i * rows, rows), :]
            shape = (chunk_steps, batch, tile)
            span = pl.ds(i * chunk_steps, chunk_steps)
            gate_pre = jnp.dot(lhs, wbuf[0, :, cols], preferred_element_type=F32).reshape(shape)
            cand_pre = jnp.dot(lhs, wbuf[1, :, cols], preferred_element_type=F32).reshape(shape)
            gate_pre = gate_pre + drive_g[span, :, cols].astype(F32)
            cand_pre = cand_pre + drive_c[span, :, cols].astype(F32)
            guess = traj[span, :, cols]
            if i == 0:
                previous = jnp.concatenate([prev0[:, cols][None], guess[:-1]], 0)
            else:
                previous = traj[pl.ds(i * chunk_steps - 1, chunk_steps), :, cols]
            update = jax.nn.sigmoid(gate_pre)
            candidate = jnp.tanh(cand_pre)
            keep = 1.0 - update
            mapped = keep * previous + update * candidate
            jacobian = (
                keep
                + update * keep * (candidate - previous) * diag[0, :, cols][None]
                + update * (1.0 - candidate * candidate) * diag[1, :, cols][None]
            )
            offset = mapped - jacobian * previous
            missing = guess - mapped
            ssq[:, cols] += jnp.sum(missing * missing, axis=0)
            product = carry[0, :, cols]
            state = carry[1, :, cols]
            for s in range(chunk_steps):
                product = jacobian[s] * product
                state = jacobian[s] * state + offset[s]
                prod[i * chunk_steps + s, :, cols] = product
                out[i * chunk_steps + s, :, cols] = state
            carry[0, :, cols] = product
            carry[1, :, cols] = state

    for i in range(chunks):
        relay(nz - 1, i)
        compute(i)

    def pm_copy():
        return remote(carry, partner_map, pm_sem.at[0], pm_sem.at[1], partner)

    pm_copy().start()
    mine = ssq[:, pl.ds(0, 128)]
    for j in range(1, width // 128):
        mine = mine + ssq[:, pl.ds(j * 128, 128)]
    tsums[t] = mine

    def ts_copy(d):
        slot = tsums.at[t]
        return remote(slot, slot, ts_send.at[d - 1], ts_recv.at[d - 1], (z, lax.rem(t + d, nt)))

    def ts_arrival(d):
        slot = tsums.at[lax.rem(t + nt - d, nt)]
        return remote(slot, slot, ts_send.at[d - 1], ts_recv.at[d - 1], partner)

    for d in range(1, nt):
        ts_copy(d).start()

    def m_copy(dq):
        slot = maps.at[chip]
        return remote(
            slot, slot, m_send.at[dq - 1], m_recv.at[dq - 1], (z, 2 * cmod(chip + dq) + core)
        )

    def m_arrival(dq):
        slot = maps.at[cmod(chip - dq)]
        return remote(slot, slot, m_send.at[dq - 1], m_recv.at[dq - 1], partner)

    pm_copy().wait()
    is_second = core == 1
    p_mine, s_mine, p_other, s_other = carry[0], carry[1], partner_map[0], partner_map[1]
    p_late = jnp.where(is_second, p_mine, p_other)
    s_early = jnp.where(is_second, s_other, s_mine)
    s_late = jnp.where(is_second, s_mine, s_other)
    maps[chip, 0] = p_mine * p_other
    maps[chip, 1] = p_late * s_early + s_late
    for dq in range(1, nc):
        m_copy(dq).start()

    for d in range(1, nt):
        ts_arrival(d).wait_recv()
    plane = tsums[0]
    for k in range(1, nt):
        plane = plane + tsums[k]
    zsums[z] = plane

    def zs_copy(d):
        slot = zsums.at[z]
        return remote(slot, slot, zs_send.at[d - 1], zs_recv.at[d - 1], (zmod(z + d), t))

    def zs_arrival(d):
        slot = zsums.at[zmod(z - d)]
        return remote(slot, slot, zs_send.at[d - 1], zs_recv.at[d - 1], partner)

    for d in range(1, nz):
        zs_copy(d).start()

    for dq in range(1, nc):
        m_arrival(dq).wait_recv()
    entry = init[...]
    for q in range(nc):
        entry = jnp.where(q < chip, maps[q, 0] * entry + maps[q, 1], entry)
    entry = jnp.where(is_second, p_other * entry + s_other, entry)
    carry_entry = entry
    prev0[...] = carry_entry

    @pl.loop(0, steps)
    def _(s):
        out[s] = prod[s] * prev0[...] + out[s]

    for d in range(1, nz):
        zs_arrival(d).wait_recv()
    whole = zsums[0]
    for k in range(1, nz):
        whole = whole + zsums[k]
    total[...] = whole

    for d in range(1, nz):
        zs_copy(d).wait_send()
        for g in range(2):
            z_copy(d, g).wait_send()
            for dq in range(1, nc):
                x_copy(d, g, dq).wait_send()
            for dq in range(nc):
                c_copy(d, g, dq, core).wait_send()
    for d in range(1, nt):
        ts_copy(d).wait_send()
    for dq in range(1, nc):
        m_copy(dq).wait_send()
    for i in range(chunks):
        for source in range(nz):
            @pl.when(jnp.logical_and(source <= z, z < nz - 1))
            def _():
                a_copy(0, source, i).wait_send()

            @pl.when(jnp.logical_and(source >= z, z > 0))
            def _():
                a_copy(1, source, i).wait_send()


def local(nz, nt, trajectory, initial, drive_gate, drive_candidate, gate_weight, candidate_weight):
    steps, batch, width = trajectory.shape
    nc = nt // 2
    full = gate_weight.shape[1]
    chunks = 4
    tile = min(256, width)
    dma = pltpu.SemaphoreType.DMA
    vmem = pl.BlockSpec(memory_space=pltpu.VMEM)
    hbm = pl.BlockSpec(memory_space=pl.ANY)
    states, total = pl.pallas_call(
        functools.partial(kernel, nz, nt, chunks, tile),
        out_shape=(
            jax.ShapeDtypeStruct((steps, batch, width), F32),
            jax.ShapeDtypeStruct((batch, 128), F32),
        ),
        in_specs=[vmem, vmem, vmem, vmem, hbm, hbm],
        out_specs=(vmem, vmem),
        scratch_shapes=[
            pltpu.VMEM((2, full, width), BF16),
            pltpu.VMEM((steps * batch, full), BF16),
            pltpu.VMEM((batch, width), F32),
            pltpu.VMEM((2, batch, width), F32),
            pltpu.VMEM((steps, batch, width), F32),
            pltpu.VMEM((2, batch, width), F32),
            pltpu.VMEM((batch, width), F32),
            pltpu.VMEM((2, batch, width), F32),
            pltpu.VMEM((nc, 2, batch, width), F32),
            pltpu.VMEM((nt, batch, 128), F32),
            pltpu.VMEM((nz, batch, 128), F32),
            dma((2,)),
            dma((2, nz - 1)),
            dma((2, nz - 1)),
            dma((2, nz - 1, nc - 1)),
            dma((2, nz - 1, nc - 1)),
            dma((2, nz - 1, nc)),
            dma((2, nz - 1, nc)),
            dma((2, nz, chunks)),
            dma((nz, chunks)),
            dma((2,)),
            dma((2,)),
            dma((nc - 1,)),
            dma((nc - 1,)),
            dma((nt - 1,)),
            dma((nt - 1,)),
            dma((nz - 1,)),
            dma((nz - 1,)),
        ],
        compiler_params=pltpu.CompilerParams(
            collective_id=0, has_side_effects=True, vmem_limit_bytes=56 * 2**20
        ),
    )(trajectory, initial, drive_gate, drive_candidate, gate_weight, candidate_weight)
    entries = trajectory.size * nz * nt
    residual_norm = jnp.sqrt(jnp.sum(total) / entries + 1e-06)
    return (states, residual_norm)


def solution(mesh):
    placed = (
        P("tm", None, "chan"),
        P(None, "chan"),
        P("tm", None, "chan"),
        P("tm", None, "chan"),
        P("chan", None),
        P("chan", None),
    )
    body = functools.partial(local, mesh.shape["chan"], mesh.shape["tm"])
    return jax.shard_map(
        body, mesh=mesh, in_specs=placed, out_specs=(P("tm", None, "chan"), P()), check_vma=False
    )
```
